32 devices in a mesh: gx: 4 (over z), gy: 2 (over y), gz: 4 (over x, core).
Axes of the slice: x: 2, y: 2, z: 4, core: 2. Of those that a mesh axis runs over, the one named last changes fastest.
Arguments:
- right_side: float32 [256, 128, 256], P('gx', 'gy', 'gz'), may hold values from -6 to 6
- guess: float32 [256, 128, 256], P('gx', 'gy', 'gz'), may hold values from -6 to 6
Outputs:
- solution: float32 [256, 128, 256], P('gx', 'gy', 'gz')
- residual: float32 [256, 128, 256], P('gx', 'gy', 'gz')
The draws below stay inside these ranges and needn't reach their ends.
All inputs are finite; a program needn't handle non-finite values.
Results may differ from the reference program's by a relative error of at most 0.0003.
Values sent between devices are 32-bit elements.
A program may use at most 256 MiB of HBM per device.

```python
import jax
import jax.numpy as jnp
from jax import lax

LEVELS = 7
COARSE_SWEEPS = 4
NX = 256
NY = 128
NZ = 256


def level_of(stream_key, dims, split, low, largest):
    def one(axis_at, blocks):
        heights = jax.random.uniform(jax.random.fold_in(jax.random.fold_in(stream_key, 6), axis_at), (blocks,), jnp.float32, low / len(split), largest / len(split))
        return jnp.repeat(jnp.exp(heights), dims[axis_at] // blocks).reshape((-1,) + (1,) * (len(dims) - axis_at - 1))

    loudness = one(*split[0])
    for cut in split[1:]:
        loudness = loudness * one(*cut)
    return loudness


def bell_draw(key, shape, deviation, most, cuts=(), held_as=jnp.bfloat16):
    array = deviation * jax.random.normal(key, shape, jnp.float32)
    if cuts:
        array = array * level_of(key, shape, cuts, -0.22, 0.18)
    return jnp.clip(array, -most, most).astype(held_as)


def setup_inputs(seed: int = 0) -> dict:
    streams_of = jax.random.split(jax.random.key(seed), 3)
    right_side = bell_draw(streams_of[0], (NX, NY, NZ), 1.0, 6.0, ((0, 4), (1, 2), (2, 4)), jnp.float32)
    guess = bell_draw(streams_of[1], (NX, NY, NZ), 1.0, 6.0, ((0, 4), (1, 2), (2, 4)), jnp.float32)
    return dict(right_side=right_side, guess=guess)


def face_total(padded):
    total = padded[2:, 1:-1, 1:-1] + padded[:-2, 1:-1, 1:-1]
    total = total + padded[1:-1, 2:, 1:-1] + padded[1:-1, :-2, 1:-1]
    total = total + padded[1:-1, 1:-1, 2:] + padded[1:-1, 1:-1, :-2]
    return total


def neighbours(field):
    return face_total(jnp.pad(field, 1))


def walls(index, total):
    return (index == 0).astype(jnp.float32) + (index == total - 1).astype(jnp.float32)


def geometry(shape):
    first = lax.iota(jnp.int32, shape[0])[:, None, None]
    second = lax.iota(jnp.int32, shape[1])[None, :, None]
    third = lax.iota(jnp.int32, shape[2])[None, None, :]
    parity = (first + second + third) % 2
    diagonal = 6.0 + walls(first, shape[0]) + walls(second, shape[1]) + walls(third, shape[2])
    return parity == 0, parity == 1, diagonal


def half_sweep(field, source, colour, diagonal, scale):
    updated = (scale * source + neighbours(field)) / diagonal
    return jnp.where(colour, updated, field)


def residual_of(field, source, diagonal, inverse):
    return source - (diagonal * field - neighbours(field)) * inverse


def restrict(remainder):
    shape = remainder.shape
    grouped = remainder.reshape(shape[0] // 2, 2, shape[1] // 2, 2, shape[2] // 2, 2)
    return jnp.sum(grouped, axis=(1, 3, 5)) * 0.125


def odd_pad(field):
    for axis in range(3):
        count = field.shape[axis]
        lowest = -lax.slice_in_dim(field, 0, 1, axis=axis)
        highest = -lax.slice_in_dim(field, count - 1, count, axis=axis)
        field = jnp.concatenate([lowest, field, highest], axis=axis)
    return field


def prolong(padded):
    centre = padded[1:-1, 1:-1, 1:-1]
    below_first = 0.25 * (padded[:-2, 1:-1, 1:-1] - centre)
    above_first = 0.25 * (padded[2:, 1:-1, 1:-1] - centre)
    below_second = 0.25 * (padded[1:-1, :-2, 1:-1] - centre)
    above_second = 0.25 * (padded[1:-1, 2:, 1:-1] - centre)
    below_third = 0.25 * (padded[1:-1, 1:-1, :-2] - centre)
    above_third = 0.25 * (padded[1:-1, 1:-1, 2:] - centre)
    along_first = jnp.stack([below_first, above_first], axis=1)[:, :, :, None, :, None]
    along_second = jnp.stack([below_second, above_second], axis=2)[:, None, :, :, :, None]
    along_third = jnp.stack([below_third, above_third], axis=3)[:, None, :, None, :, :]
    fine = centre[:, None, :, None, :, None] + along_first + along_second + along_third
    shape = centre.shape
    return fine.reshape(2 * shape[0], 2 * shape[1], 2 * shape[2])


def cycle(field, source, level):
    red, black, diagonal = geometry(source.shape)
    scale = 4.0 ** level
    if level == LEVELS - 1:
        for sweep_index in range(COARSE_SWEEPS):
            field = half_sweep(field, source, red, diagonal, scale)
            field = half_sweep(field, source, black, diagonal, scale)
        return field
    field = half_sweep(field, source, red, diagonal, scale)
    field = half_sweep(field, source, black, diagonal, scale)
    coarse = restrict(residual_of(field, source, diagonal, 0.25 ** level))
    correction = cycle(jnp.zeros_like(coarse), coarse, level + 1)
    field = field + prolong(odd_pad(correction))
    field = half_sweep(field, source, red, diagonal, scale)
    return half_sweep(field, source, black, diagonal, scale)


def reference(right_side, guess):
    solution = cycle(guess, right_side, 0)
    red, black, diagonal = geometry(right_side.shape)
    return solution, residual_of(solution, right_side, diagonal, 1.0)
```

```python
import jax
import jax.numpy as jnp
from jax import lax
from jax.experimental import pallas as pl
from jax.experimental.pallas import tpu as pltpu
from jax.sharding import PartitionSpec as P

LEVELS = 7
COARSE_SWEEPS = 4
GATHER = 3
LANES = 128
AXES = ("gx", "gy", "gz")
HIGHEST = lax.Precision.HIGHEST


def rows_of(count):
    return max(8, count)


def lane_iota(rows):
    return lax.broadcasted_iota(jnp.int32, (rows, LANES), 1)


def row_iota(rows):
    return lax.broadcasted_iota(jnp.int32, (rows, LANES), 0)


def loop(count, body):
    if count == 1:
        body(0)
    else:
        def step(i, carry):
            body(i)
            return carry
        lax.fori_loop(0, count, step, 0)


class Level:
    def __init__(self, number, dims, places, counts, v, s, w, d):
        self.number, self.dims, self.places, self.counts = number, dims, places, counts
        self.v, self.s, self.w, self.d = v, s, w, d
        self.rows = rows_of(dims[1])
        self.scale = 4.0 ** number
        self.inverse = 0.25 ** number
        self.chunk = min(dims[0], max(2, 32 * 8 // self.rows))

    def prepare(self):
        x, y, z = self.dims
        row, lane = row_iota(self.rows), lane_iota(self.rows)
        valid = (row < y) & (lane < z)
        at_y, at_z = self.places[1] * y + row, self.places[2] * z + lane
        one = lambda at, total: (at == 0).astype(jnp.float32) + (at == total - 1).astype(jnp.float32)
        base = 6.0 + one(at_y, self.counts[1] * y) + one(at_z, self.counts[2] * z)
        for wall in range(2):
            self.d[wall] = jnp.where(valid, base + wall, 0.0)
            for parity in range(2):
                self.w[2 * wall + parity] = jnp.where(valid & ((row + lane) % 2 == parity), 1.0 / (base + wall), 0.0)
        self.v[...] = jnp.zeros_like(self.v)

    def wall(self, plane):
        at = self.places[0] * self.dims[0] + plane
        last = self.counts[0] * self.dims[0] - 1
        if isinstance(at, int):
            return int(at in (0, last))
        return jnp.where((at == 0) | (at == last), 1, 0)

    def total(self, start, face):
        count, rows, z = self.chunk, self.rows, self.dims[2]
        slab = self.v[pl.ds(start, count + 2), pl.ds(8, rows), :]
        centre = slab[1:-1]
        total = slab[2:] + slab[:-2]
        total = total + self.v[pl.ds(start + 1, count), pl.ds(9, rows), :] + self.v[pl.ds(start + 1, count), pl.ds(7, rows), :]
        lane = lane_iota(rows)
        out = []
        for i in range(count):
            c = centre[i]
            if face is None:
                z_sum = pltpu.roll(c, 1, 1) + pltpu.roll(c, LANES - 1, 1)
            else:
                g = pltpu.roll(face[...], LANES - (start + i), 1)
                if z != 64:
                    g_high = pltpu.roll(g, LANES + z - 64, 1) if z < 64 else g
                    high = jnp.where(lane == z, g_high, c)
                else:
                    high = jnp.where(lane == 64, g, c)
                z_sum = jnp.where(lane == 0, g, pltpu.roll(c, 1, 1)) + pltpu.roll(high, LANES - 1, 1)
            out.append(total[i] + z_sum)
        return out, [centre[i] for i in range(count)]

    def sweep(self, colour, face=None, zero=False):
        def body(step):
            start = step * self.chunk
            if not zero:
                totals, centres = self.total(start, face)
            results = []
            for i in range(self.chunk):
                weight = self.w[2 * self.wall(start + i) + (i + colour) % 2]
                given = self.scale * self.s[start + i]
                if zero:
                    results.append(given * weight)
                else:
                    results.append(jnp.where(weight > 0, (given + totals[i]) * weight, centres[i]))
            for i in range(self.chunk):
                self.v[start + i + 1, pl.ds(8, self.rows), :] = results[i]
        loop(self.dims[0] // self.chunk, body)

    def remainder(self, start, face):
        totals, centres = self.total(start, face)
        out = []
        for i in range(self.chunk):
            d = self.d[self.wall(start + i)]
            out.append(jnp.where(d > 0, self.s[start + i] - (d * centres[i] - totals[i]) * self.inverse, 0.0))
        return out

    def restrict_to(self, target, pairs, face=None):
        rows, z = self.rows, self.dims[2]
        coarse_rows = rows_of(self.dims[1] // 2)
        half = self.chunk // 2
        source_lane = lax.broadcasted_iota(jnp.int32, (LANES, LANES), 0)
        target_lane = lax.broadcasted_iota(jnp.int32, (LANES, LANES), 1)
        halve = jnp.where((source_lane // 2 == target_lane) & (source_lane < z), 0.125, 0.0)
        if rows < 16:
            pairs[...] = jnp.zeros_like(pairs)

        def first(step):
            r = self.remainder(step * self.chunk, face)
            for i in range(half):
                pairs[step * half + i, pl.ds(0, rows), :] = r[2 * i] + r[2 * i + 1]
        loop(self.dims[0] // self.chunk, first)

        planes = self.dims[0] // 2
        many = min(planes, max(1, 256 // coarse_rows))

        def second(step):
            at = pl.ds(step * many, many)
            q = pairs[at, pl.ds(0, coarse_rows, stride=2), :] + pairs[at, pl.ds(1, coarse_rows, stride=2), :]
            q = jnp.dot(q.reshape(many * coarse_rows, LANES), halve, precision=HIGHEST, preferred_element_type=jnp.float32)
            target[at] = q.reshape(many, coarse_rows, LANES)
        loop(planes // many, second)

    def reflect(self):
        x, y, z = self.dims
        v = self.v

        def low_x():
            v[0] = -v[1]

        def high_x():
            v[x + 1] = -v[x]

        def low_y():
            for_all = pl.ds(1, x)
            v[for_all, pl.ds(7, 1), :] = -v[for_all, pl.ds(8, 1), :]

        def high_y():
            for_all = pl.ds(1, x)
            v[for_all, pl.ds(8 + y, 1), :] = -v[for_all, pl.ds(7 + y, 1), :]

        for axis, low, high in ((0, low_x, high_x), (1, low_y, high_y)):
            if isinstance(self.counts[axis], int) and isinstance(self.places[axis], int):
                low()
                high()
            else:
                pl.when(self.places[axis] == 0)(low)
                pl.when(self.places[axis] == self.counts[axis] - 1)(high)


def lift(v, dims, places, counts, fine, spread, high_lane, face=None):
    x, y, z = dims
    rows = rows_of(y)
    k = lax.broadcasted_iota(jnp.int32, (LANES, LANES), 0)
    f = lax.broadcasted_iota(jnp.int32, (LANES, LANES), 1)
    inside = f < 2 * z
    own = ((f // 2 == k) & inside).astype(jnp.float32)
    beside = ((f // 2 + 2 * (f % 2) - 1 == k) & inside & (k < z)).astype(jnp.float32)
    low_wall = jnp.where(places[2] == 0, 1.0, 0.0)
    high_wall = jnp.where(places[2] == counts[2] - 1, 1.0, 0.0)
    at_low, at_high = f == 0, f == 2 * z - 1
    beside = beside + jnp.where(at_low & (k == 0), -low_wall, 0.0) + jnp.where(at_low & (k == LANES - 1), 1.0 - low_wall, 0.0)
    beside = beside + jnp.where(at_high & (k == z - 1), -high_wall, 0.0) + jnp.where(at_high & (k == high_lane), 1.0 - high_wall, 0.0)
    both = 0.25 * (own + beside)
    own = 0.25 * own
    tall = rows + 16
    lane = lane_iota(rows)
    valid = row_iota(rows) < y

    def first(plane):
        spread[plane] = jnp.dot(v[plane], own, precision=HIGHEST, preferred_element_type=jnp.float32)

    group = 2
    loop((x + 2) // group, lambda step: [first(step * group + i) for i in range(group)])

    def second(plane):
        e = v[plane + 1, pl.ds(8, rows), :]
        if face is not None:
            e = jnp.where(lane < z, e, pltpu.roll(pltpu.roll(face[...], LANES - plane, 1), LANES - 1, 1))
        centre = jnp.dot(e, both, precision=HIGHEST, preferred_element_type=jnp.float32)
        ys = (spread[plane + 1, pl.ds(7, rows), :], spread[plane + 1, pl.ds(9, rows), :])
        for up_x in range(2):
            xs = centre + spread[plane + 2 * up_x, pl.ds(8, rows), :]
            for up_y in range(2):
                q = xs + ys[up_y]
                if y < rows:
                    q = jnp.where(valid, q, 0.0)
                at = (2 * plane + up_x + 1, pl.ds(8 + up_y, rows, stride=2), slice(None))
                fine.v[at] = fine.v[at] + q

    loop(x // group, lambda step: [second(step * group + i) for i in range(group)])


def solve_kernel(counts, blocks, coarse, uses, refs):
    right_side, guess, out_v, out_r = refs[:4]
    refs = list(refs[4:])
    take = lambda: refs.pop(0)
    places = tuple(lax.axis_index(axis) for axis in AXES)
    levels = []
    for number, dims in enumerate(blocks[:GATHER]):
        levels.append(Level(number, dims, places, counts, take(), take(), take(), take()))
    for number, dims in enumerate(coarse):
        levels.append(Level(GATHER + number, dims, (0, 0, 0), (1, 1, 1), take(), take(), take(), take()))
    exchange = [(take(), take(), take(), take(), take()) for _ in range(GATHER)]
    pairs = [take() for _ in range(LEVELS - 1)]
    spreads = [take() for _ in range(LEVELS - 1)]
    block_s, block_v, packet, packets, gather_send, gather_recv = refs

    for level in levels:
        level.prepare()
    for number in range(GATHER):
        exchange[number][4][...] = jnp.zeros_like(exchange[number][4])
    z0 = blocks[0][2]
    top = levels[0]

    def load(x):
        top.v[x + 1, pl.ds(8, top.rows), pl.ds(0, z0)] = guess[x]
        top.s[x] = jnp.concatenate([right_side[x], jnp.zeros((top.rows, LANES - z0), jnp.float32)], axis=1)
    loop(blocks[0][0] // 4, lambda step: [load(4 * step + i) for i in range(4)])

    turn = [0] * GATHER
    sent = []

    def swap(number):
        level = levels[number]
        out, into, send, recv, face = exchange[number]
        n, v, (x, y, z) = turn[number], level.v, level.dims
        turn[number] += 1
        out[n, 0, pl.ds(0, y)] = v[x, pl.ds(8, y), :]
        out[n, 1, pl.ds(0, y)] = v[1, pl.ds(8, y), :]
        out[n, 2, pl.ds(0, x)] = v[pl.ds(1, x), 7 + y, :]
        out[n, 3, pl.ds(0, x)] = v[pl.ds(1, x), 8, :]
        lane = lane_iota(y)
        many = min(x, 8)

        def columns(step, carry):
            last, leading = carry
            for i in range(many):
                plane = step * many + i
                c = v[plane + 1, pl.ds(8, y), :]
                last = jnp.where(lane == plane, pltpu.roll(c, plane + LANES - (z - 1), 1), last)
                leading = jnp.where(lane == plane + 64, pltpu.roll(c, plane + 64, 1), leading)
            return last, leading
        zero = jnp.zeros((y, LANES), jnp.float32)
        last, leading = lax.fori_loop(0, x // many, columns, (zero, zero))
        out[n, 4, pl.ds(0, y)] = last
        out[n, 5, pl.ds(0, y)] = leading

        copies = []
        for axis in range(3):
            for way in range(2):
                side = 2 * axis + way
                other = places[axis] + (1 - 2 * way)
                copy = pltpu.make_async_remote_copy(
                    src_ref=out.at[n, side], dst_ref=into.at[n, side],
                    send_sem=send.at[n, side], recv_sem=recv.at[n, side],
                    device_id={AXES[axis]: other}, device_id_type=pl.DeviceIdType.MESH)
                has_target = other < counts[axis] if way == 0 else other >= 0
                has_origin = places[axis] > 0 if way == 0 else places[axis] < counts[axis] - 1
                pl.when(has_target)(copy.start)
                sent.append((has_target, copy))
                copies.append((has_origin, copy))

        def land(side):
            got = into.at[n, side]
            if side == 0:
                v[0, pl.ds(8, y), :] = got[pl.ds(0, y)]
            elif side == 1:
                v[x + 1, pl.ds(8, y), :] = got[pl.ds(0, y)]
            elif side == 2:
                v[pl.ds(1, x), 7, :] = got[pl.ds(0, x)]
            elif side == 3:
                v[pl.ds(1, x), 8 + y, :] = got[pl.ds(0, x)]
            elif side == 4:
                face[...] = jnp.where(lane < 64, got[pl.ds(0, y)], face[...])
            else:
                face[...] = jnp.where(lane >= 64, got[pl.ds(0, y)], face[...])
        for side, (has_origin, copy) in enumerate(copies):
            @pl.when(has_origin)
            def _(side=side, copy=copy):
                copy.wait_recv()
                land(side)
        return face

    for number in range(GATHER):
        level = levels[number]
        if number == 0:
            level.sweep(0, swap(0))
        else:
            level.sweep(0, zero=True)
        level.sweep(1, swap(number))
        target = levels[number + 1].s if number + 1 < GATHER else block_s
        level.restrict_to(target, pairs[number], swap(number))

    bx, by, bz = blocks[GATHER]
    packed = block_s[0]
    for x in range(1, bx):
        packed = packed + pltpu.roll(block_s[x], x * bz, 1)
    packet[...] = packed
    total = counts[0] * counts[1] * counts[2]
    me = (places[0] * counts[1] + places[1]) * counts[2] + places[2]

    def gather_copy(source, target, offset):
        return pltpu.make_async_remote_copy(
            src_ref=packet, dst_ref=packets.at[source],
            send_sem=gather_send.at[target], recv_sem=gather_recv.at[source],
            device_id=(target // (counts[1] * counts[2]), target // counts[2] % counts[1], target % counts[2]),
            device_id_type=pl.DeviceIdType.MESH)

    def post(offset, carry):
        gather_copy(me, lax.rem(me + offset, total), offset).start()
        return carry
    lax.fori_loop(1, total, post, 0)
    packets[me] = packed

    def arrive(offset, carry):
        source = lax.rem(me + total - offset, total)
        gather_copy(source, lax.rem(me + offset, total), offset).wait_recv()
        return carry
    lax.fori_loop(1, total, arrive, 0)
    whole = levels[GATHER]
    lane = lane_iota(by)

    def unpack(step):
        px, py = step // counts[1], step % counts[1]
        for x in range(bx):
            row = jnp.zeros((by, LANES), jnp.float32)
            for pz in range(counts[2]):
                shifted = pltpu.roll(packets[step * counts[2] + pz], (pz * bz - x * bz) % LANES, 1)
                row = jnp.where((lane >= pz * bz) & (lane < pz * bz + bz), shifted, row)
            whole.s[px * bx + x, pl.ds(pl.multiple_of(py * by, 8), by), :] = row
    loop(counts[0] * counts[1], unpack)

    for number in range(GATHER, LEVELS - 1):
        level = levels[number]
        level.sweep(0, zero=True)
        level.sweep(1)
        level.restrict_to(levels[number + 1].s, pairs[number])
    level = levels[LEVELS - 1]
    level.sweep(0, zero=True)
    level.sweep(1)
    for _ in range(COARSE_SWEEPS - 1):
        level.sweep(0)
        level.sweep(1)
    for number in reversed(range(GATHER, LEVELS - 1)):
        level, below = levels[number], levels[number + 1]
        below.reflect()
        lift(below.v, below.dims, (0, 0, 0), (1, 1, 1), level, spreads[number], below.dims[2])
        level.sweep(0)
        level.sweep(1)

    whole.reflect()
    shift = lax.rem(LANES - places[2] * bz, LANES)
    for x in range(bx + 2):
        part = whole.v[places[0] * bx + x, pl.ds(pl.multiple_of(places[1] * by, 8), by + 16), :]
        block_v[x] = pltpu.roll(part, shift, 1)
    lift(block_v, blocks[GATHER], places, counts, levels[GATHER - 1], spreads[GATHER - 1], bz)
    for number in reversed(range(GATHER)):
        level = levels[number]
        level.sweep(0, swap(number))
        level.sweep(1, swap(number))
        face = swap(number)
        if number > 0:
            level.reflect()
            lift(level.v, level.dims, places, counts, levels[number - 1], spreads[number - 1], 63, face)

    def finish(step):
        r = top.remainder(step * top.chunk, face)
        for i in range(top.chunk):
            at = step * top.chunk + i
            out_r[at] = r[i][:, :z0]
            out_v[at] = top.v[at + 1, pl.ds(8, top.rows), pl.ds(0, z0)]
    loop(blocks[0][0] // top.chunk, finish)

    for has_target, copy in sent:
        pl.when(has_target)(copy.wait_send)

    def leave(offset, carry):
        gather_copy(me, lax.rem(me + offset, total), offset).wait_send()
        return carry
    lax.fori_loop(1, total, leave, 0)


def solution(mesh):
    counts = tuple(mesh.shape[axis] for axis in AXES)

    def per_device(right_side, guess):
        shape = right_side.shape
        blocks = [tuple(side >> level for side in shape) for level in range(GATHER + 1)]
        whole = tuple(side * count for side, count in zip(blocks[GATHER], counts))
        coarse = [tuple(side >> level for side in whole) for level in range(LEVELS - GATHER)]
        grids = blocks[:GATHER] + coarse
        scratch = []
        vmem = lambda *dims: scratch.append(pltpu.VMEM(dims, jnp.float32))
        for x, y, z in grids:
            vmem(x + 2, rows_of(y) + 16, LANES)
            vmem(x, rows_of(y), LANES)
            vmem(4, rows_of(y), LANES)
            vmem(2, rows_of(y), LANES)
        for number, (x, y, z) in enumerate(blocks[:GATHER]):
            turns = 6 if number == 0 else 5
            side = max(x, y)
            vmem(turns, 6, side, LANES)
            vmem(turns, 6, side, LANES)
            scratch.append(pltpu.SemaphoreType.DMA((turns, 6)))
            scratch.append(pltpu.SemaphoreType.DMA((turns, 6)))
            vmem(y, LANES)
        for x, y, z in grids[:-1]:
            vmem(x // 2, max(16, y), LANES)
        for number in range(LEVELS - 1):
            x, y, z = blocks[number + 1] if number < GATHER else grids[number + 1]
            vmem(x + 2, rows_of(y) + 16, LANES)
        bx, by, bz = blocks[GATHER]
        vmem(bx, by, LANES)
        vmem(bx + 2, by + 16, LANES)
        vmem(by, LANES)
        total = counts[0] * counts[1] * counts[2]
        vmem(total, by, LANES)
        scratch.append(pltpu.SemaphoreType.DMA((total,)))
        scratch.append(pltpu.SemaphoreType.DMA((total,)))

        def kernel(*refs):
            solve_kernel(counts, blocks, coarse, None, refs)

        whole_block = pl.BlockSpec(memory_space=pltpu.VMEM)
        return pl.pallas_call(
            kernel,
            out_shape=(jax.ShapeDtypeStruct(shape, jnp.float32),) * 2,
            in_specs=[whole_block] * 2,
            out_specs=(whole_block,) * 2,
            scratch_shapes=scratch,
            compiler_params=pltpu.CompilerParams(has_side_effects=True, vmem_limit_bytes=60 * 2**20),
            name="vcycle",
        )(right_side, guess)

    spec = P(*AXES)
    return jax.shard_map(per_device, mesh=mesh, in_specs=(spec, spec), out_specs=(spec, spec), check_vma=False)
```
